32 devices in a mesh: dp: 1 (over z), cfg: 4 (over y), tp: 8 (over x, core).
Axes of the slice: x: 4, y: 4, z: 1, core: 2. Of those that a mesh axis runs over, the one named last changes fastest.
The devices are a block of a 4x4x8 slice.
Arguments:
- hidden: bfloat16 [4, 4096, 1152], P(('dp', 'cfg'))
- caption: bfloat16 [4, 120, 1152], P(('dp', 'cfg'))
- cap_len: int32 [4], P(('dp', 'cfg'))
- t_block: bfloat16 [2, 6912], P('dp')
- t_embed: bfloat16 [2, 1152], P('dp')
- x_t: float32 [2, 128, 128, 4], P('dp')
- alpha_bar: float32 [2, 2], P('dp')
- mod_table: bfloat16 [2, 6, 1152], replicated
- w_qkv: bfloat16 [2, 1152, 3, 16, 72], P(None, None, None, 'tp')
- w_proj: bfloat16 [2, 16, 72, 1152], P(None, 'tp')
- w_cq: bfloat16 [2, 1152, 16, 72], P(None, None, 'tp')
- w_ckv: bfloat16 [2, 1152, 2, 16, 72], P(None, None, None, 'tp')
- w_cproj: bfloat16 [2, 16, 72, 1152], P(None, 'tp')
- w_fc1: bfloat16 [2, 1152, 4608], P(None, None, 'tp')
- w_fc2: bfloat16 [2, 4608, 1152], P(None, 'tp')
- final_table: bfloat16 [2, 1152], replicated
- w_out: bfloat16 [1152, 32], replicated
- b_out: bfloat16 [32], replicated
Outputs:
- output: float32 [2, 128, 128, 4], P('dp')
All inputs are finite; a program needn't handle non-finite values.
Results may differ from the reference program's by a relative error of at most 0.0132671.
Values are sent between devices in bfloat16 or wider.
A program may use at most 768 MiB of HBM per device.

```python
import jax
import jax.numpy as jnp
from jax import lax

BATCH_SIZE = 2
LATENT_SIDE = 128
MODEL_DIM = 1152
NUM_HEADS = 16
TEXT_LEN = 120
HIDDEN_FF = 4608

NUM_TOKENS = (LATENT_SIDE // 2) * (LATENT_SIDE // 2)
HEAD_DIM = MODEL_DIM // NUM_HEADS
GUIDANCE = 4.5
LN_EPS = 1e-6


def setup_inputs(seed: int = 0, part: int = 0) -> dict:
    part_keys = jax.random.split(jax.random.fold_in(jax.random.key(seed), part), 10)
    weight_keys = jax.random.split(jax.random.key(seed + 1), 11)
    total_rows = 2 * BATCH_SIZE
    common = jax.random.normal(part_keys[0], (total_rows, 1, MODEL_DIM), jnp.float32)
    tok_noise = jax.random.normal(part_keys[1], (total_rows, NUM_TOKENS, MODEL_DIM), jnp.float32)
    hidden = common + tok_noise
    cap_mean = jax.random.normal(part_keys[2], (total_rows, 1, MODEL_DIM), jnp.float32)
    caption = cap_mean + jax.random.normal(part_keys[3], (total_rows, TEXT_LEN, MODEL_DIM), jnp.float32)
    len_keys = jax.random.split(part_keys[4], 2)
    cond_len = jax.random.randint(len_keys[0], (BATCH_SIZE,), TEXT_LEN // 4, TEXT_LEN + 1)
    uncond_len = jax.random.randint(len_keys[1], (BATCH_SIZE,), 1, TEXT_LEN // 16 + 2)
    cap_len = jnp.concatenate([cond_len.at[0].set(TEXT_LEN), uncond_len]).astype(jnp.int32)
    t_block = 0.5 * jax.random.normal(part_keys[5], (BATCH_SIZE, 6 * MODEL_DIM), jnp.float32)
    t_embed = 0.5 * jax.random.normal(part_keys[6], (BATCH_SIZE, MODEL_DIM), jnp.float32)
    x_t = jax.random.normal(part_keys[7], (BATCH_SIZE, LATENT_SIDE, LATENT_SIDE, 4), jnp.float32)
    abar_t = jax.random.uniform(part_keys[8], (BATCH_SIZE,), jnp.float32, 0.15, 0.6)
    abar_gap = jax.random.uniform(part_keys[9], (BATCH_SIZE,), jnp.float32, 0.1, 0.3)
    alpha_bar = jnp.stack([abar_t, abar_t + abar_gap], axis=1)
    dim_scale = MODEL_DIM ** -0.5
    ff_scale = HIDDEN_FF ** -0.5
    mod_table = 0.5 * jax.random.normal(weight_keys[0], (2, 6, MODEL_DIM), jnp.float32)
    w_qkv = dim_scale * jax.random.normal(weight_keys[1], (2, MODEL_DIM, 3, NUM_HEADS, HEAD_DIM), jnp.float32)
    w_proj = dim_scale * jax.random.normal(weight_keys[2], (2, NUM_HEADS, HEAD_DIM, MODEL_DIM), jnp.float32)
    w_cq = dim_scale * jax.random.normal(weight_keys[3], (2, MODEL_DIM, NUM_HEADS, HEAD_DIM), jnp.float32)
    w_ckv = dim_scale * jax.random.normal(weight_keys[4], (2, MODEL_DIM, 2, NUM_HEADS, HEAD_DIM), jnp.float32)
    w_cproj = dim_scale * jax.random.normal(weight_keys[5], (2, NUM_HEADS, HEAD_DIM, MODEL_DIM), jnp.float32)
    w_fc1 = dim_scale * jax.random.normal(weight_keys[6], (2, MODEL_DIM, HIDDEN_FF), jnp.float32)
    w_fc2 = ff_scale * jax.random.normal(weight_keys[7], (2, HIDDEN_FF, MODEL_DIM), jnp.float32)
    final_table = 0.5 * jax.random.normal(weight_keys[8], (2, MODEL_DIM), jnp.float32)
    w_out = dim_scale * jax.random.normal(weight_keys[9], (MODEL_DIM, 32), jnp.float32)
    b_out = 0.3 * jax.random.normal(weight_keys[10], (32,), jnp.float32)
    return {
        'hidden': hidden.astype(jnp.bfloat16),
        'caption': caption.astype(jnp.bfloat16),
        'cap_len': cap_len,
        't_block': t_block.astype(jnp.bfloat16),
        't_embed': t_embed.astype(jnp.bfloat16),
        'x_t': x_t,
        'alpha_bar': alpha_bar,
        'mod_table': mod_table.astype(jnp.bfloat16),
        'w_qkv': w_qkv.astype(jnp.bfloat16),
        'w_proj': w_proj.astype(jnp.bfloat16),
        'w_cq': w_cq.astype(jnp.bfloat16),
        'w_ckv': w_ckv.astype(jnp.bfloat16),
        'w_cproj': w_cproj.astype(jnp.bfloat16),
        'w_fc1': w_fc1.astype(jnp.bfloat16),
        'w_fc2': w_fc2.astype(jnp.bfloat16),
        'final_table': final_table.astype(jnp.bfloat16),
        'w_out': w_out.astype(jnp.bfloat16),
        'b_out': b_out.astype(jnp.bfloat16),
    }


def layer_norm(values):
    mean_val = jnp.mean(values, axis=-1, keepdims=True)
    centered = values - mean_val
    variance = jnp.mean(centered * centered, axis=-1, keepdims=True)
    return centered * lax.rsqrt(variance + LN_EPS)


def attend(queries, key_vecs, values, key_mask):
    def one_head(head_in):
        q_head, k_head, v_head = head_in
        scores = jnp.dot(q_head, k_head.T, preferred_element_type=jnp.float32) * HEAD_DIM ** -0.5
        scores = jnp.where(key_mask[None, :], scores, -1e30)
        attn_prob = jax.nn.softmax(scores, axis=-1).astype(jnp.bfloat16)
        return jnp.dot(attn_prob, v_head, preferred_element_type=jnp.float32).astype(jnp.bfloat16)
    per_head = lax.map(one_head, (jnp.swapaxes(queries, 0, 1), jnp.swapaxes(key_vecs, 0, 1), jnp.swapaxes(values, 0, 1)))
    return jnp.swapaxes(per_head, 0, 1)


def block_row(residual, caption_row, key_mask, t_mods, layer_w):
    mod_tab, w_qkv, w_proj, w_cq, w_ckv, w_cproj, w_fc1, w_fc2 = layer_w
    mod_rows = mod_tab.astype(jnp.float32) + t_mods
    all_keys = jnp.ones((NUM_TOKENS,), jnp.bool_)
    attn_in = (layer_norm(residual) * (1.0 + mod_rows[1]) + mod_rows[0]).astype(jnp.bfloat16)
    qkv_out = jnp.dot(attn_in, w_qkv.reshape(MODEL_DIM, 3 * MODEL_DIM), preferred_element_type=jnp.float32)
    qkv_out = qkv_out.astype(jnp.bfloat16).reshape(NUM_TOKENS, 3, NUM_HEADS, HEAD_DIM)
    self_o = attend(qkv_out[:, 0], qkv_out[:, 1], qkv_out[:, 2], all_keys)
    self_proj = jnp.dot(self_o.reshape(NUM_TOKENS, MODEL_DIM), w_proj.reshape(MODEL_DIM, MODEL_DIM), preferred_element_type=jnp.float32).astype(jnp.bfloat16)
    residual = residual + mod_rows[2] * self_proj.astype(jnp.float32)
    cross_q = jnp.dot(residual.astype(jnp.bfloat16), w_cq.reshape(MODEL_DIM, MODEL_DIM), preferred_element_type=jnp.float32)
    cross_q = cross_q.astype(jnp.bfloat16).reshape(NUM_TOKENS, NUM_HEADS, HEAD_DIM)
    cross_kv = jnp.dot(caption_row, w_ckv.reshape(MODEL_DIM, 2 * MODEL_DIM), preferred_element_type=jnp.float32)
    cross_kv = cross_kv.astype(jnp.bfloat16).reshape(TEXT_LEN, 2, NUM_HEADS, HEAD_DIM)
    cross_o = attend(cross_q, cross_kv[:, 0], cross_kv[:, 1], key_mask)
    cross_proj = jnp.dot(cross_o.reshape(NUM_TOKENS, MODEL_DIM), w_cproj.reshape(MODEL_DIM, MODEL_DIM), preferred_element_type=jnp.float32).astype(jnp.bfloat16)
    residual = residual + cross_proj.astype(jnp.float32)
    mlp_in = (layer_norm(residual) * (1.0 + mod_rows[4]) + mod_rows[3]).astype(jnp.bfloat16)
    mlp_hidden = jax.nn.gelu(jnp.dot(mlp_in, w_fc1, preferred_element_type=jnp.float32), approximate=True).astype(jnp.bfloat16)
    mlp_out = jnp.dot(mlp_hidden, w_fc2, preferred_element_type=jnp.float32).astype(jnp.bfloat16)
    return residual + mod_rows[5] * mlp_out.astype(jnp.float32)


def reference(hidden, caption, cap_len, t_block, t_embed, x_t, alpha_bar, mod_table, w_qkv, w_proj, w_cq, w_ckv, w_cproj, w_fc1, w_fc2, final_table, w_out, b_out):
    t_rows = jnp.tile(t_block.astype(jnp.float32).reshape(BATCH_SIZE, 6, MODEL_DIM), (2, 1, 1))
    emb_rows = jnp.tile(t_embed.astype(jnp.float32), (2, 1))
    layer_ws = (mod_table, w_qkv, w_proj, w_cq, w_ckv, w_cproj, w_fc1, w_fc2)

    def per_row(row_in):
        hidden_row, caption_row, len_row, t_mods, emb_row = row_in
        key_mask = jnp.arange(TEXT_LEN) < len_row

        def layer_step(residual, layer_w):
            return block_row(residual, caption_row, key_mask, t_mods, layer_w), None

        residual, scan_out = lax.scan(layer_step, hidden_row.astype(jnp.float32), layer_ws)
        shift_scale = final_table.astype(jnp.float32) + emb_row[None, :]
        final_in = (layer_norm(residual) * (1.0 + shift_scale[1]) + shift_scale[0]).astype(jnp.bfloat16)
        out_tok = jnp.dot(final_in, w_out, preferred_element_type=jnp.float32) + b_out.astype(jnp.float32)
        grid_side = LATENT_SIDE // 2
        patches = out_tok.reshape(grid_side, grid_side, 2, 2, 8)[:, :, :, :, :4]
        return patches.transpose(0, 2, 1, 3, 4).reshape(LATENT_SIDE, LATENT_SIDE, 4)

    eps_rows = lax.map(per_row, (hidden, caption, cap_len, t_rows, emb_rows))
    eps_cond = eps_rows[:BATCH_SIZE]
    eps_uncond = eps_rows[BATCH_SIZE:]
    guided = eps_uncond + GUIDANCE * (eps_cond - eps_uncond)
    abar_t = alpha_bar[:, 0][:, None, None, None]
    abar_prev = alpha_bar[:, 1][:, None, None, None]
    x_zero = (x_t - jnp.sqrt(1.0 - abar_t) * guided) / jnp.sqrt(abar_t)
    return jnp.sqrt(abar_prev) * x_zero + jnp.sqrt(1.0 - abar_prev) * guided
```

```python
import functools

import jax
import jax.numpy as jnp
from jax import lax
from jax.experimental import pallas as pl
from jax.experimental.pallas import tpu as pltpu
from jax.sharding import PartitionSpec as P

GUIDANCE = 4.5
LN_EPS = 1e-6
LOG2E = 1.4426950408889634
MESH = pl.DeviceIdType.MESH
BF16 = jnp.bfloat16
F32 = jnp.float32
K_ROWS = 512
F_ROWS = 768


def layer_norm(values):
    mean_val = jnp.mean(values, axis=-1, keepdims=True)
    centered = values - mean_val
    variance = jnp.mean(centered * centered, axis=-1, keepdims=True)
    return centered * lax.rsqrt(variance + LN_EPS)


def dot32(spec, left, right):
    return jnp.einsum(spec, left, right, preferred_element_type=F32)


ROW_W = ('kv', 'proj', 'cq', 'cproj')
GRID_W = ('fc1', 'fc2')
EAST = {'kv': False, 'proj': True, 'cq': True, 'cproj': False, 'fc1': True, 'fc2': False}


class Wires:
    def __init__(self, send_sem, recv_sem):
        self.send_sem, self.recv_sem, self.ids, self.sent = send_sem, recv_sem, {}, []

    def idx(self, key):
        return self.ids.setdefault(key, len(self.ids))

    def copy(self, key, src, dst, dev):
        k = self.idx(key)
        return pltpu.make_async_remote_copy(src_ref=src, dst_ref=dst, send_sem=self.send_sem.at[k],
                                            recv_sem=self.recv_sem.at[k], device_id=dev, device_id_type=MESH)

    def start(self, key, src, dst, dev):
        self.sent.append((key, src, dst, dev))
        self.copy(key, src, dst, dev).start()

    def arrived(self, key, region, dev):
        self.copy(key, region, region, dev).wait_recv()

    def drain(self):
        for item in self.sent:
            self.copy(*item).wait_send()


def attn_kernel(n_tp, n_cfg, head_dim, scale, norm, a_in, w_ref, mod_ref, kv_in, proj_in, cq_in, cproj_in, fc1_in, fc2_in,
                out_o, kv_g, proj_g, cq_g, cproj_g, fc1_g, fc2_g,
                o_buf, a_buf, q_ref, k_ref, v_ref, send_sem, recv_sem, o_send, o_recv, loc_sem, a_sem):
    me = lax.axis_index('tp')
    row = lax.axis_index('cfg')
    east, west, opp = lax.rem(me + 2, n_tp), lax.rem(me + n_tp - 2, n_tp), lax.rem(me + 4, n_tp)
    mate = me + 1 - 2 * lax.rem(me, 2)
    flip = lambda idx: idx + 1 - 2 * lax.rem(idx, 2)
    north, south, far = lax.rem(row + 1, n_cfg), lax.rem(row + n_cfg - 1, n_cfg), lax.rem(row + 2, n_cfg)
    to_east, to_west, to_mate = {'tp': east}, {'tp': west}, {'tp': mate}
    to_north, to_south = {'cfg': north}, {'cfg': south}
    src = dict(kv=kv_in, proj=proj_in, cq=cq_in, cproj=cproj_in, fc1=fc1_in, fc2=fc2_in)
    full = dict(kv=kv_g, proj=proj_g, cq=cq_g, cproj=cproj_g, fc1=fc1_g, fc2=fc2_g)
    wires = Wires(send_sem, recv_sem)
    n_chunk, _, chunk_rows = o_buf.shape
    n_heads = v_ref.shape[0]
    width = n_heads * head_dim

    barrier = pltpu.get_barrier_semaphore()
    for step in range(1, n_tp):
        pl.semaphore_signal(barrier, inc=1, device_id={'tp': lax.rem(me + step, n_tp)}, device_id_type=MESH)
    for dev in (to_north, to_south):
        pl.semaphore_signal(barrier, inc=1, device_id=dev, device_id_type=MESH)
    pl.semaphore_wait(barrier, n_tp + 1)

    def o_copy(step):
        there = lax.rem(me + 1 + step, n_tp)
        return pltpu.make_async_remote_copy(src_ref=o_buf.at[step], dst_ref=out_o.at[me], send_sem=o_send.at[step],
                                            recv_sem=o_recv.at[step], device_id={'tp': there}, device_id_type=MESH)

    o_local = pltpu.make_async_copy(o_buf.at[n_tp - 1], out_o.at[me], loc_sem)

    def spread_y(name, shard, tag):
        part = full[name].at[shard, row]
        wires.start(('y', name, tag, 'N'), part, part, to_north)
        wires.start(('y', name, tag, 'S'), part, part, to_south)

    def hand_mate(key, part):
        wires.start(('d',) + key, part, part, to_mate)

    def ev_first():
        for name in GRID_W:
            wires.start(('x', name, 'E'), src[name].at[row], full[name].at[me, row], to_east)
            wires.start(('x', name, 'W'), src[name].at[row], full[name].at[me, row], to_west)
        for name in GRID_W + ROW_W:
            wires.start(('own', name), src[name], full[name].at[me], to_mate)

    def ev_x_near(name):
        wires.arrived(('x', name, 'E'), full[name].at[west, row], to_west)
        wires.arrived(('x', name, 'W'), full[name].at[east, row], to_east)
        part = full[name].at[west if EAST[name] else east, row]
        wires.start(('xf', name), part, part, to_east if EAST[name] else to_west)
        for shard, tag in ((west, 'w'), (east, 'e')):
            spread_y(name, shard, tag)
            hand_mate((name, tag, 0), full[name].at[shard, row])

    def ev_row_first():
        for name in ROW_W:
            wires.start(('x', name, 'E'), src[name], full[name].at[me], to_east)
            wires.start(('x', name, 'W'), src[name], full[name].at[me], to_west)

    def ev_x_opp():
        for name in GRID_W:
            wires.arrived(('xf', name), full[name].at[opp, row], to_west if EAST[name] else to_east)
            spread_y(name, opp, 'o')
            hand_mate((name, 'o', 0), full[name].at[opp, row])

    def ev_y(shard, tag):
        for name in GRID_W:
            wires.arrived(('y', name, tag, 'N'), full[name].at[shard, south], to_south)
            wires.arrived(('y', name, tag, 'S'), full[name].at[shard, north], to_north)
            part = full[name].at[shard, south if EAST[name] else north]
            wires.start(('yf', name, tag), part, part, to_north if EAST[name] else to_south)
            hand_mate((name, tag, 1), full[name].at[shard, south])
            hand_mate((name, tag, 2), full[name].at[shard, north])

    def ev_row_near():
        for name in ROW_W:
            wires.arrived(('x', name, 'E'), full[name].at[west], to_west)
            wires.arrived(('x', name, 'W'), full[name].at[east], to_east)
            part = full[name].at[west if EAST[name] else east]
            wires.start(('xf', name), part, part, to_east if EAST[name] else to_west)
            hand_mate((name, 'w', 0), full[name].at[west])
            hand_mate((name, 'e', 0), full[name].at[east])
        for name in GRID_W + ROW_W:
            wires.arrived(('own', name), full[name].at[mate], to_mate)
            wires.start(('back', name), full[name].at[mate], full[name].at[mate], to_mate)

    def ev_row_opp():
        for name in ROW_W:
            wires.arrived(('xf', name), full[name].at[opp], to_west if EAST[name] else to_east)
            hand_mate((name, 'o', 0), full[name].at[opp])

    def ev_y_far(shard, tag):
        for name in GRID_W:
            wires.arrived(('yf', name, tag), full[name].at[shard, far], to_south if EAST[name] else to_north)
            hand_mate((name, tag, 3), full[name].at[shard, far])

    def ev_second():
        ev_x_near('fc2')
        ev_row_first()

    ev_first()
    loads = [pltpu.make_async_copy(a_in.at[pl.ds(i * chunk_rows, chunk_rows)], a_buf.at[i], a_sem.at[i]) for i in range(n_chunk)]
    for load in loads:
        load.start()
    for load in loads:
        load.wait()
    v_ref[:, head_dim:] = jnp.ones((n_heads, v_ref.shape[1] - head_dim, v_ref.shape[2]), BF16)

    def project(at, carry):
        act = a_buf[at]
        if norm:
            act = (layer_norm(act.astype(F32)) * (1.0 + mod_ref[1:2]) + mod_ref[0:1]).astype(BF16)
        cols = pl.ds(pl.multiple_of(at * chunk_rows, chunk_rows), chunk_rows)
        across = (((1,), (1,)), ((), ()))
        q_ref[:, cols] = lax.dot_general(w_ref[0], act, across, preferred_element_type=F32).astype(BF16)
        k_ref[cols] = lax.dot_general(act, w_ref[1], across, preferred_element_type=F32).astype(BF16)
        vals = lax.dot_general(w_ref[2], act, across, preferred_element_type=F32).astype(BF16)
        for h in range(n_heads):
            v_ref[h, :head_dim, cols] = vals[h * head_dim:(h + 1) * head_dim]
        if norm:
            pl.when(at == 5)(lambda: ev_x_near('fc1'))
        return carry

    lax.fori_loop(0, n_chunk, project, 0)
    if norm:
        ev_second()
        events = {0: ev_x_opp, 2: lambda: ev_y(west, 'w'), 3: lambda: ev_y(east, 'e'), 5: ev_row_near}
    else:
        ev_x_near('fc1')
        events = {0: ev_second, 1: ev_x_opp, 3: lambda: ev_y(west, 'w'), 4: lambda: ev_y(east, 'e'), 6: ev_row_near}
    row_ids = lax.broadcasted_iota(jnp.int32, (width, chunk_rows), 0)

    def attend(step, carry):
        chunk = lax.rem(me + 1 + step, n_tp)
        q_all = q_ref[:, pl.ds(pl.multiple_of(chunk * chunk_rows, chunk_rows), chunk_rows)]
        queries = [jnp.where((row_ids >= h * head_dim) & (row_ids < (h + 1) * head_dim), q_all, 0) for h in range(n_heads)]
        units = [(h, j) for j in range(k_ref.shape[0] // K_ROWS) for h in range(n_heads)]
        score = lambda unit: jnp.dot(k_ref[pl.ds(unit[1] * K_ROWS, K_ROWS)], queries[unit[0]], preferred_element_type=F32)
        top, mixed = [None] * n_heads, [None] * n_heads
        scores = score(units[0])
        for at, (h, j) in enumerate(units):
            ahead = score(units[at + 1]) if at + 1 < len(units) else None
            peak = jnp.max(scores, axis=0, keepdims=True)
            if j:
                peak = jnp.maximum(peak, top[h])
                fade = jnp.exp2((top[h] - peak) * (scale * LOG2E))
            top[h] = peak
            probs = jnp.exp2((scores - peak) * (scale * LOG2E)).astype(BF16)
            term = jnp.dot(v_ref[h, :, pl.ds(j * K_ROWS, K_ROWS)], probs, preferred_element_type=F32)
            mixed[h] = mixed[h] * fade + term if j else term
            scores = ahead
        outs = [part[:head_dim] / part[head_dim:head_dim + 1] for part in mixed]
        o_buf[step] = jnp.concatenate(outs, axis=0).astype(BF16)

        @pl.when(step < n_tp - 1)
        def _():
            o_copy(step).start()
        for when, event in events.items():
            pl.when(step == when)(event)
        return carry

    lax.fori_loop(0, n_chunk, attend, 0)
    o_local.start()
    ev_y(opp, 'o')
    ev_row_opp()
    for shard, tag in ((west, 'w'), (east, 'e'), (opp, 'o')):
        ev_y_far(shard, tag)
    for name in GRID_W:
        for shard, tag in ((west, 'w'), (east, 'e'), (opp, 'o')):
            for part, at_row in enumerate((row, south, north, far)):
                wires.arrived(('d', name, tag, part), full[name].at[flip(shard), at_row], to_mate)
    for name in ROW_W:
        for shard, tag in ((west, 'w'), (east, 'e'), (opp, 'o')):
            wires.arrived(('d', name, tag, 0), full[name].at[flip(shard)], to_mate)
    for name in GRID_W + ROW_W:
        wires.arrived(('back', name), full[name].at[me], to_mate)
    wires.drain()
    for step in range(n_tp - 1):
        origin = lax.rem(me + n_tp - 1 - step, n_tp)
        o_copy(step).wait_send()
        pltpu.make_async_remote_copy(src_ref=out_o.at[origin], dst_ref=out_o.at[origin], send_sem=o_send.at[step],
                                     recv_sem=o_recv.at[step], device_id={'tp': origin}, device_id_type=MESH).wait_recv()
    o_local.wait()


N_WIRES = 6 + 12 + 6 + 12 + 6 + 24 + 12 + 6


def attend_and_gather(mesh, layer, norm, n_heads, act, w_t, mods, kv, shards):
    n_tp, n_cfg = mesh.shape['tp'], mesh.shape['cfg']
    n_tok, dim = act.shape
    width = w_t.shape[1]
    head_dim = width // n_heads
    vmem = pl.BlockSpec(memory_space=pltpu.VMEM)
    hbm = pl.BlockSpec(memory_space=pl.ANY)
    sem = pltpu.SemaphoreType.DMA
    out_shape = [jax.ShapeDtypeStruct((n_tp, width, n_tok // n_tp), BF16)]
    out_shape += [jax.ShapeDtypeStruct((n_tp,) + shard.shape, BF16) for shard in (kv,) + shards]
    return pl.pallas_call(
        functools.partial(attn_kernel, n_tp, n_cfg, head_dim, head_dim ** -0.5, norm),
        out_shape=out_shape,
        in_specs=[hbm, vmem, vmem] + [hbm] * 6,
        out_specs=[hbm] * 7,
        scratch_shapes=[pltpu.VMEM((n_tp, width, n_tok // n_tp), BF16), pltpu.VMEM((n_tp, n_tok // n_tp, dim), BF16),
                        pltpu.VMEM((width, n_tok), BF16), pltpu.VMEM((n_tok, width), BF16), pltpu.VMEM((n_heads, head_dim + 8, n_tok), BF16),
                        sem((N_WIRES,)), sem((N_WIRES,)), sem((n_tp - 1,)), sem((n_tp - 1,)), sem, sem((n_tp,))],
        compiler_params=pltpu.CompilerParams(collective_id=layer, has_side_effects=True, vmem_limit_bytes=60 << 20),
        name=f'attend_gather_{layer}',
    )(act, w_t, mods, kv, *shards)


def mlp_kernel(res_ref, mod_ref, w1_ref, w2_ref, out_ref, next_ref, a_buf, total):
    at = pl.program_id(0)

    @pl.when(at == 0)
    def _():
        a_buf[...] = (layer_norm(res_ref[...]) * (1.0 + mod_ref[1:2]) + mod_ref[0:1]).astype(BF16)
        total[...] = jnp.zeros_like(total)
    hidden = lax.dot_general(a_buf[...], w1_ref[...], (((1,), (1,)), ((), ())), preferred_element_type=F32)
    hidden = jax.nn.gelu(hidden, approximate=True).astype(BF16)
    total[...] += jnp.dot(hidden, w2_ref[...], preferred_element_type=F32)

    @pl.when(at == pl.num_programs(0) - 1)
    def _():
        out = res_ref[...] + mod_ref[2:3] * total[...].astype(BF16).astype(F32)
        out_ref[...] = out
        next_ref[...] = (layer_norm(out) * (1.0 + mod_ref[4:5]) + mod_ref[3:4]).astype(BF16)


def mlp(residual, mods, w1, w2):
    n_own, dim = residual.shape
    whole = lambda shape: pl.BlockSpec(shape, lambda at: (0, 0))
    block = pl.BlockSpec((F_ROWS, dim), lambda at: (at, 0))
    return pl.pallas_call(
        mlp_kernel,
        grid=(w1.shape[0] // F_ROWS,),
        out_shape=[jax.ShapeDtypeStruct((n_own, dim), F32), jax.ShapeDtypeStruct((n_own, dim), BF16)],
        in_specs=[whole((n_own, dim)), whole(mods.shape), block, block],
        out_specs=[whole((n_own, dim)), whole((n_own, dim))],
        scratch_shapes=[pltpu.VMEM((n_own, dim), BF16), pltpu.VMEM((n_own, dim), F32)],
        compiler_params=pltpu.CompilerParams(vmem_limit_bytes=48 << 20),
        cost_estimate=pl.CostEstimate(flops=4 * n_own * dim * w1.shape[0], bytes_accessed=4 * dim * w1.shape[0], transcendentals=0),
        name='norm_mlp',
    )(residual, mods, w1, w2)


def final_kernel(n_tp, n_cfg, n_img, eps_ref, x_ref, co_ref, out_ref, pair_buf, send_buf, pair_send, pair_recv, send_sem, recv_sem):
    me = lax.axis_index('tp')
    row = lax.axis_index('cfg')
    pair, up, down = lax.rem(row + n_img, n_cfg), lax.rem(row + 1, n_cfg), lax.rem(row + n_cfg - 1, n_cfg)
    image = lax.rem(row, n_img)
    barrier = pltpu.get_barrier_semaphore()
    pl.semaphore_signal(barrier, inc=1, device_id={'cfg': pair}, device_id_type=MESH)
    for step in range(n_tp):
        tp = lax.rem(me + step, n_tp)
        if step:
            pl.semaphore_signal(barrier, inc=1, device_id={'tp': tp}, device_id_type=MESH)
        pl.semaphore_signal(barrier, inc=1, device_id={'cfg': down, 'tp': tp}, device_id_type=MESH)
    pl.semaphore_wait(barrier, 2 * n_tp)
    swap = pltpu.make_async_remote_copy(src_ref=eps_ref, dst_ref=pair_buf, send_sem=pair_send, recv_sem=pair_recv,
                                        device_id={'cfg': pair}, device_id_type=MESH)
    swap.start()
    swap.wait()
    is_cond = row < n_img
    mine, other = eps_ref[...], pair_buf[...]
    cond, uncond = jnp.where(is_cond, mine, other), jnp.where(is_cond, other, mine)
    guided = uncond + GUIDANCE * (cond - uncond)
    x_zero = (x_ref[...] - co_ref[0:1] * guided) / co_ref[1:2]
    result = co_ref[2:3] * x_zero + co_ref[3:4] * guided
    send_buf[...] = result
    out_ref[image, me] = result

    def chunk_copy(step, ring, origin, img, dev):
        k = step * 2 + ring
        return pltpu.make_async_remote_copy(src_ref=send_buf, dst_ref=out_ref.at[img, origin], send_sem=send_sem.at[k],
                                            recv_sem=recv_sem.at[k], device_id=dev, device_id_type=MESH)

    for ring in range(2):
        for step in range(1 - ring, n_tp):
            tp = lax.rem(me + step, n_tp)
            chunk_copy(step, ring, me, image, {'cfg': up, 'tp': tp} if ring else {'tp': tp}).start()
    for ring in range(2):
        for step in range(1 - ring, n_tp):
            origin = lax.rem(me + n_tp - step, n_tp)
            img = lax.rem(down, n_img) if ring else image
            dev = {'cfg': down, 'tp': origin} if ring else {'tp': origin}
            chunk_copy(step, ring, origin, img, dev).wait_recv()
            chunk_copy(step, ring, origin, img, dev).wait_send()


def final_step(mesh, eps, x_own, coef, n_img):
    n_tp, n_cfg = mesh.shape['tp'], mesh.shape['cfg']
    vmem = pl.BlockSpec(memory_space=pltpu.VMEM)
    sem = pltpu.SemaphoreType.DMA
    return pl.pallas_call(
        functools.partial(final_kernel, n_tp, n_cfg, n_img),
        out_shape=jax.ShapeDtypeStruct((n_img, n_tp) + eps.shape, F32),
        in_specs=[vmem] * 3,
        out_specs=vmem,
        scratch_shapes=[pltpu.VMEM(eps.shape, F32), pltpu.VMEM(eps.shape, F32), sem, sem, sem((2 * n_tp,)), sem((2 * n_tp,))],
        compiler_params=pltpu.CompilerParams(collective_id=16, has_side_effects=True),
        name='guide_and_share',
    )(eps, x_own, coef)


def gather_kernel(n_tp, x_ref, out_ref, send_sem, recv_sem, loc_sem):
    me = lax.axis_index('tp')
    east, west, opp = lax.rem(me + 2, n_tp), lax.rem(me + n_tp - 2, n_tp), lax.rem(me + 4, n_tp)
    flip = lambda idx: idx + 1 - 2 * lax.rem(idx, 2)
    mate = flip(me)
    to_east, to_west, to_mate = {'tp': east}, {'tp': west}, {'tp': mate}
    half = x_ref.shape[0] // 2
    barrier = pltpu.get_barrier_semaphore()
    for dev in (to_east, to_west, to_mate):
        pl.semaphore_signal(barrier, inc=1, device_id=dev, device_id_type=MESH)
    pl.semaphore_wait(barrier, 3)
    wires = Wires(send_sem, recv_sem)
    low, high = pl.ds(0, half), pl.ds(half, half)
    for tag, cut in (('l', low), ('h', high)):
        order = (('E', to_east), ('W', to_west)) if tag == 'l' else (('W', to_west), ('E', to_east))
        for side, dev in order:
            wires.start((side, tag), x_ref.at[cut], out_ref.at[me, cut], dev)
    wires.start(('own',), x_ref, out_ref.at[me], to_mate)
    local = pltpu.make_async_copy(x_ref, out_ref.at[me], loc_sem)
    local.start()
    wires.arrived(('E', 'l'), out_ref.at[west, low], to_west)
    part = out_ref.at[west, low]
    wires.start(('fE',), part, part, to_east)
    wires.start(('d', 'wl'), part, part, to_mate)
    wires.arrived(('W', 'h'), out_ref.at[east, high], to_east)
    part = out_ref.at[east, high]
    wires.start(('fW',), part, part, to_west)
    wires.start(('d', 'eh'), part, part, to_mate)
    for key, tag, part, dev in ((('E', 'h'), 'wh', out_ref.at[west, high], to_west), (('W', 'l'), 'el', out_ref.at[east, low], to_east),
                                (('fE',), 'ol', out_ref.at[opp, low], to_west), (('fW',), 'oh', out_ref.at[opp, high], to_east)):
        wires.arrived(key, part, dev)
        wires.start(('d', tag), part, part, to_mate)
    for shard, tag in ((west, 'w'), (east, 'e'), (opp, 'o')):
        wires.arrived(('d', tag + 'l'), out_ref.at[flip(shard), low], to_mate)
        wires.arrived(('d', tag + 'h'), out_ref.at[flip(shard), high], to_mate)
    wires.arrived(('own',), out_ref.at[mate], to_mate)
    wires.drain()
    local.wait()


def gather_tokens(mesh, layer, part):
    n_tp = mesh.shape['tp']
    sem = pltpu.SemaphoreType.DMA
    return pl.pallas_call(
        functools.partial(gather_kernel, n_tp),
        out_shape=jax.ShapeDtypeStruct((n_tp,) + part.shape, BF16),
        in_specs=[pl.BlockSpec(memory_space=pltpu.VMEM)],
        out_specs=pl.BlockSpec(memory_space=pl.ANY),
        scratch_shapes=[sem((13,)), sem((13,)), sem],
        compiler_params=pltpu.CompilerParams(collective_id=8 + layer, has_side_effects=True),
        name=f'gather_tokens_{layer}',
    )(part)


def solution(mesh):
    row_spec = P(('dp', 'cfg'))
    part_spec = P('dp')
    in_specs = (row_spec, row_spec, row_spec, part_spec, part_spec, part_spec, part_spec, P(),
                P(None, None, None, 'tp'), P(None, 'tp'), P(None, None, 'tp'), P(None, None, None, 'tp'),
                P(None, 'tp'), P(None, None, 'tp'), P(None, 'tp'), P(), P(), P())
    n_tp, n_cfg = mesh.shape['tp'], mesh.shape['cfg']

    def local_step(hidden, caption, cap_len, t_block, t_embed, x_t, alpha_bar, mod_table, w_qkv, w_proj, w_cq, w_ckv, w_cproj, w_fc1, w_fc2, final_table, w_out, b_out):
        _, n_tok, dim = hidden.shape
        n_layers, n_heads, head_dim = w_proj.shape[:3]
        width = n_heads * head_dim
        n_own = n_tok // n_tp
        n_text = caption.shape[1]
        n_img = t_block.shape[0]
        image = lax.axis_index('cfg') % n_img
        me = lax.axis_index('tp')
        t_rows = lax.dynamic_index_in_dim(t_block, image, keepdims=False).astype(F32).reshape(6, dim)
        emb_row = lax.dynamic_index_in_dim(t_embed, image, keepdims=False).astype(F32)
        key_mask = (jnp.arange(n_text) < cap_len[0])[None, None, :]
        residual = lax.dynamic_slice_in_dim(hidden[0], me * n_own, n_own).astype(F32)
        all_mods = mod_table.astype(F32) + t_rows[None]
        final_mods = final_table.astype(F32) + emb_row[None, :]
        attn_in = hidden[0]
        for layer in range(n_layers):
            mods = all_mods[layer]
            if layer:
                attn_in = gather_tokens(mesh, layer, next_in).reshape(n_tok, dim)
            w_t = w_qkv[layer].transpose(1, 2, 3, 0).reshape(3, width, dim)
            kv = dot32('td,dshe->shet', caption[0], w_ckv[layer]).astype(BF16).reshape(2 * n_heads, head_dim, n_text)
            f_rows = w_fc2.shape[1] // n_cfg
            shards = (w_proj[layer].reshape(width, dim), w_cq[layer].reshape(dim, width).T, w_cproj[layer].reshape(width, dim),
                      w_fc1[layer].T.reshape(n_cfg, f_rows, dim), w_fc2[layer].reshape(n_cfg, f_rows, dim))
            o_all, kv_all, g_proj, g_cq, g_cproj, g_fc1, g_fc2 = attend_and_gather(mesh, layer, layer == 0, n_heads, attn_in, w_t, mods, kv, shards)
            self_out = dot32('kn,kd->nd', o_all.reshape(n_tp * width, n_own), g_proj.reshape(n_tp * width, dim)).astype(BF16)
            residual = residual + mods[2] * self_out.astype(F32)
            cross_q = dot32('nd,hed->hne', residual.astype(BF16), g_cq.reshape(n_tp * n_heads, head_dim, dim)).astype(BF16)
            kv_all = kv_all.reshape(n_tp, 2, n_heads, head_dim, n_text)
            cross_k = kv_all[:, 0].reshape(n_tp * n_heads, head_dim, n_text)
            cross_v = kv_all[:, 1].reshape(n_tp * n_heads, head_dim, n_text)
            scores = dot32('hne,het->hnt', cross_q, cross_k) * head_dim ** -0.5
            scores = jnp.where(key_mask, scores, -1e30)
            probs = jax.nn.softmax(scores, axis=-1).astype(BF16)
            cross_o = dot32('hnt,het->nhe', probs, cross_v).astype(BF16)
            cross_out = dot32('nk,kd->nd', cross_o.reshape(n_own, n_tp * width), g_cproj.reshape(n_tp * width, dim)).astype(BF16)
            residual = residual + cross_out.astype(F32)
            after = all_mods[layer + 1, :2] if layer + 1 < n_layers else final_mods
            mlp_mods = jnp.concatenate([mods[3:6], after, jnp.zeros((3, dim), F32)], axis=0)
            n_ff = g_fc1.shape[0] * g_fc1.shape[1] * g_fc1.shape[2]
            residual, next_in = mlp(residual, mlp_mods, g_fc1.reshape(n_ff, dim), g_fc2.reshape(n_ff, dim))
        side = x_t.shape[1]
        grid = side // 2
        n_own_rows = n_own // grid
        out_tok = dot32('nd,dc->cn', next_in, w_out) + b_out.astype(F32)[:, None]
        eps = out_tok.reshape(2, 2, 8, n_own_rows, grid)[:, :, :4]
        place = (jnp.arange(side)[None, None, :] == 2 * jnp.arange(grid)[None, :, None] + jnp.arange(2)[:, None, None]).astype(F32)
        eps = jnp.einsum('pqcij,qjx->ipcx', eps, place, precision=lax.Precision.HIGHEST, preferred_element_type=F32)
        eps = eps.reshape(n_own_rows * 2 * 4, side)
        x_rows = x_t.transpose(0, 1, 3, 2).reshape(n_img, n_tp, n_own_rows * 2 * 4, side)
        x_own = lax.dynamic_slice(x_rows, (image, me, 0, 0), (1, 1) + x_rows.shape[2:])[0, 0]
        abar = lax.dynamic_index_in_dim(alpha_bar, image, keepdims=False)
        coef = jnp.stack([jnp.sqrt(1.0 - abar[0]), jnp.sqrt(abar[0]), jnp.sqrt(abar[1]), jnp.sqrt(1.0 - abar[1])])
        coef = jnp.broadcast_to(jnp.concatenate([coef, coef])[:, None], (8, side))
        x_prev = final_step(mesh, eps, x_own, coef, n_img)
        return x_prev.reshape(n_img, side, 4, side).transpose(0, 1, 3, 2)

    return jax.shard_map(local_step, mesh=mesh, in_specs=in_specs, out_specs=part_spec, check_vma=False)
```

```python
import functools

import jax
import jax.numpy as jnp
from jax import lax
from jax.experimental import pallas as pl
from jax.experimental.pallas import tpu as pltpu
from jax.sharding import PartitionSpec as P

GUIDANCE = 4.5
LN_EPS = 1e-6
LOG2E = 1.4426950408889634
MESH = pl.DeviceIdType.MESH
BF16 = jnp.bfloat16
F32 = jnp.float32
K_ROWS = 512
SPAN = 4
F_ROWS = 512


def layer_norm(values):
    mean_val = jnp.mean(values, axis=-1, keepdims=True)
    centered = values - mean_val
    variance = jnp.mean(centered * centered, axis=-1, keepdims=True)
    return centered * lax.rsqrt(variance + LN_EPS)


def dot32(spec, left, right):
    return jnp.einsum(spec, left, right, preferred_element_type=F32)


ROW_W = ('kv', 'proj', 'cq', 'cproj')
GRID_W = ('fc1', 'fc2')
EAST = {'kv': False, 'proj': True, 'cq': True, 'cproj': False, 'fc1': True, 'fc2': False}


class Wires:
    def __init__(self, send_sem, recv_sem):
        self.send_sem, self.recv_sem, self.ids, self.sent = send_sem, recv_sem, {}, []

    def idx(self, key):
        return self.ids.setdefault(key, len(self.ids))

    def copy(self, key, src, dst, dev):
        k = self.idx(key)
        return pltpu.make_async_remote_copy(src_ref=src, dst_ref=dst, send_sem=self.send_sem.at[k],
                                            recv_sem=self.recv_sem.at[k], device_id=dev, device_id_type=MESH)

    def start(self, key, src, dst, dev):
        self.sent.append((key, src, dst, dev))
        self.copy(key, src, dst, dev).start()

    def arrived(self, key, region, dev):
        self.copy(key, region, region, dev).wait_recv()

    def drain(self):
        for item in self.sent:
            self.copy(*item).wait_send()


def attn_kernel(n_tp, n_cfg, head_dim, scale, norm, a_in, w_ref, mod_ref, kv_in, proj_in, cq_in, cproj_in, fc1_in, fc2_in,
                out_o, kv_g, proj_g, cq_g, cproj_g, fc1_g, fc2_g,
                o_buf, a_buf, q_ref, k_ref, v_ref, send_sem, recv_sem, o_send, o_recv, loc_sem, a_sem):
    me = lax.axis_index('tp')
    row = lax.axis_index('cfg')
    east, west, opp = lax.rem(me + 2, n_tp), lax.rem(me + n_tp - 2, n_tp), lax.rem(me + 4, n_tp)
    mate = me + 1 - 2 * lax.rem(me, 2)
    flip = lambda idx: idx + 1 - 2 * lax.rem(idx, 2)
    north, south, far = lax.rem(row + 1, n_cfg), lax.rem(row + n_cfg - 1, n_cfg), lax.rem(row + 2, n_cfg)
    to_east, to_west, to_mate = {'tp': east}, {'tp': west}, {'tp': mate}
    to_north, to_south = {'cfg': north}, {'cfg': south}
    src = dict(kv=kv_in, proj=proj_in, cq=cq_in, cproj=cproj_in, fc1=fc1_in, fc2=fc2_in)
    full = dict(kv=kv_g, proj=proj_g, cq=cq_g, cproj=cproj_g, fc1=fc1_g, fc2=fc2_g)
    wires = Wires(send_sem, recv_sem)
    n_chunk, _, chunk_rows = o_buf.shape
    n_heads = v_ref.shape[0]
    width = n_heads * head_dim

    barrier = pltpu.get_barrier_semaphore()
    for step in range(1, n_tp):
        pl.semaphore_signal(barrier, inc=1, device_id={'tp': lax.rem(me + step, n_tp)}, device_id_type=MESH)
    for dev in (to_north, to_south):
        pl.semaphore_signal(barrier, inc=1, device_id=dev, device_id_type=MESH)
    pl.semaphore_wait(barrier, n_tp + 1)

    def o_copy(step):
        there = lax.rem(me + 1 + step, n_tp)
        return pltpu.make_async_remote_copy(src_ref=o_buf.at[step], dst_ref=out_o.at[me], send_sem=o_send.at[step],
                                            recv_sem=o_recv.at[step], device_id={'tp': there}, device_id_type=MESH)

    o_local = pltpu.make_async_copy(o_buf.at[n_tp - 1], out_o.at[me], loc_sem)

    def spread_y(name, shard, tag):
        part = full[name].at[shard, row]
        wires.start(('y', name, tag, 'N'), part, part, to_north)
        wires.start(('y', name, tag, 'S'), part, part, to_south)

    def hand_mate(key, part):
        wires.start(('d',) + key, part, part, to_mate)

    def ev_first():
        for name in GRID_W:
            wires.start(('x', name, 'E'), src[name].at[row], full[name].at[me, row], to_east)
            wires.start(('x', name, 'W'), src[name].at[row], full[name].at[me, row], to_west)
        for name in GRID_W + ROW_W:
            wires.start(('own', name), src[name], full[name].at[me], to_mate)

    def ev_x_near(name):
        wires.arrived(('x', name, 'E'), full[name].at[west, row], to_west)
        wires.arrived(('x', name, 'W'), full[name].at[east, row], to_east)
        part = full[name].at[west if EAST[name] else east, row]
        wires.start(('xf', name), part, part, to_east if EAST[name] else to_west)
        for shard, tag in ((west, 'w'), (east, 'e')):
            spread_y(name, shard, tag)
            hand_mate((name, tag, 0), full[name].at[shard, row])

    def ev_row_first():
        for name in ROW_W:
            wires.start(('x', name, 'E'), src[name], full[name].at[me], to_east)
            wires.start(('x', name, 'W'), src[name], full[name].at[me], to_west)

    def ev_x_opp():
        for name in GRID_W:
            wires.arrived(('xf', name), full[name].at[opp, row], to_west if EAST[name] else to_east)
            spread_y(name, opp, 'o')
            hand_mate((name, 'o', 0), full[name].at[opp, row])

    def ev_y(shard, tag):
        for name in GRID_W:
            wires.arrived(('y', name, tag, 'N'), full[name].at[shard, south], to_south)
            wires.arrived(('y', name, tag, 'S'), full[name].at[shard, north], to_north)
            part = full[name].at[shard, south if EAST[name] else north]
            wires.start(('yf', name, tag), part, part, to_north if EAST[name] else to_south)
            hand_mate((name, tag, 1), full[name].at[shard, south])
            hand_mate((name, tag, 2), full[name].at[shard, north])

    def ev_row_near():
        for name in ROW_W:
            wires.arrived(('x', name, 'E'), full[name].at[west], to_west)
            wires.arrived(('x', name, 'W'), full[name].at[east], to_east)
            part = full[name].at[west if EAST[name] else east]
            wires.start(('xf', name), part, part, to_east if EAST[name] else to_west)
            hand_mate((name, 'w', 0), full[name].at[west])
            hand_mate((name, 'e', 0), full[name].at[east])
        for name in GRID_W + ROW_W:
            wires.arrived(('own', name), full[name].at[mate], to_mate)
            wires.start(('back', name), full[name].at[mate], full[name].at[mate], to_mate)

    def ev_row_opp():
        for name in ROW_W:
            wires.arrived(('xf', name), full[name].at[opp], to_west if EAST[name] else to_east)
            hand_mate((name, 'o', 0), full[name].at[opp])

    def ev_y_far(shard, tag):
        for name in GRID_W:
            wires.arrived(('yf', name, tag), full[name].at[shard, far], to_south if EAST[name] else to_north)
            hand_mate((name, tag, 3), full[name].at[shard, far])

    def ev_second():
        ev_x_near('fc2')
        ev_row_first()

    ev_first()
    loads = [pltpu.make_async_copy(a_in.at[pl.ds(i * chunk_rows, chunk_rows)], a_buf.at[i], a_sem.at[i]) for i in range(n_chunk)]
    for load in loads:
        load.start()
    v_ref[:, head_dim:] = jnp.ones((n_heads, v_ref.shape[1] - head_dim, v_ref.shape[2]), BF16)

    def project(at, carry):
        pltpu.make_async_copy(a_in.at[pl.ds(at * chunk_rows, chunk_rows)], a_buf.at[at], a_sem.at[at]).wait()
        act = a_buf[at]
        if norm:
            act = (layer_norm(act.astype(F32)) * (1.0 + mod_ref[1:2]) + mod_ref[0:1]).astype(BF16)
        cols = pl.ds(pl.multiple_of(at * chunk_rows, chunk_rows), chunk_rows)
        across = (((1,), (1,)), ((), ()))
        q_ref[:, cols] = lax.dot_general(w_ref[0], act, across, preferred_element_type=F32).astype(BF16)
        k_ref[cols] = lax.dot_general(act, w_ref[1], across, preferred_element_type=F32).astype(BF16)
        vals = lax.dot_general(w_ref[2], act, across, preferred_element_type=F32).astype(BF16)
        for h in range(n_heads):
            v_ref[h, :head_dim, cols] = vals[h * head_dim:(h + 1) * head_dim]
        if norm:
            pl.when(at == 3)(lambda: ev_x_near('fc1'))
        return carry

    lax.fori_loop(0, n_chunk, project, 0)
    if norm:
        ev_second()
        events = {0: ev_x_opp, 2: lambda: ev_y(west, 'w'), 3: lambda: ev_y(east, 'e'), 5: ev_row_near}
    else:
        ev_x_near('fc1')
        events = {0: ev_second, 1: ev_x_opp, 3: lambda: ev_y(west, 'w'), 4: lambda: ev_y(east, 'e'), 6: ev_row_near}
    row_ids = lax.broadcasted_iota(jnp.int32, (width, chunk_rows), 0)

    def attend(step, carry):
        chunk = lax.rem(me + 1 + step, n_tp)
        q_all = q_ref[:, pl.ds(pl.multiple_of(chunk * chunk_rows, chunk_rows), chunk_rows)]
        queries = [jnp.where((row_ids >= h * head_dim) & (row_ids < (h + 1) * head_dim), q_all, 0) for h in range(n_heads)]
        units = [(h, j) for j in range(SPAN) for h in range(n_heads)]

        def span(turn, state):
            top, mixed = list(state[:n_heads]), list(state[n_heads:])
            rows = lambda j: pl.ds(pl.multiple_of((turn * SPAN + j) * K_ROWS, K_ROWS), K_ROWS)
            score = lambda unit: jnp.dot(k_ref[rows(unit[1])], queries[unit[0]], preferred_element_type=F32)
            scores = score(units[0])
            for at, (h, j) in enumerate(units):
                ahead = score(units[at + 1]) if at + 1 < len(units) else None
                peak = jnp.maximum(jnp.max(scores, axis=0, keepdims=True), top[h])
                fade = jnp.exp2((top[h] - peak) * (scale * LOG2E))
                top[h] = peak
                probs = jnp.exp2((scores - peak) * (scale * LOG2E)).astype(BF16)
                mixed[h] = mixed[h] * fade + jnp.dot(v_ref[h, :, rows(j)], probs, preferred_element_type=F32)
                scores = ahead
            return (*top, *mixed)

        state = [jnp.full((1, chunk_rows), -jnp.inf, F32)] * n_heads + [jnp.zeros((v_ref.shape[1], chunk_rows), F32)] * n_heads
        mixed = lax.fori_loop(0, k_ref.shape[0] // (K_ROWS * SPAN), span, tuple(state))[n_heads:]
        outs = [part[:head_dim] / part[head_dim:head_dim + 1] for part in mixed]
        o_buf[step] = jnp.concatenate(outs, axis=0).astype(BF16)

        @pl.when(step < n_tp - 1)
        def _():
            o_copy(step).start()
        for when, event in events.items():
            pl.when(step == when)(event)
        return carry

    lax.fori_loop(0, n_chunk, attend, 0)
    o_local.start()
    ev_y(opp, 'o')
    ev_row_opp()
    for shard, tag in ((west, 'w'), (east, 'e'), (opp, 'o')):
        ev_y_far(shard, tag)
    for name in GRID_W:
        for shard, tag in ((west, 'w'), (east, 'e'), (opp, 'o')):
            for part, at_row in enumerate((row, south, north, far)):
                wires.arrived(('d', name, tag, part), full[name].at[flip(shard), at_row], to_mate)
    for name in ROW_W:
        for shard, tag in ((west, 'w'), (east, 'e'), (opp, 'o')):
            wires.arrived(('d', name, tag, 0), full[name].at[flip(shard)], to_mate)
    for name in GRID_W + ROW_W:
        wires.arrived(('back', name), full[name].at[me], to_mate)
    wires.drain()
    for step in range(n_tp - 1):
        origin = lax.rem(me + n_tp - 1 - step, n_tp)
        o_copy(step).wait_send()
        pltpu.make_async_remote_copy(src_ref=out_o.at[origin], dst_ref=out_o.at[origin], send_sem=o_send.at[step],
                                     recv_sem=o_recv.at[step], device_id={'tp': origin}, device_id_type=MESH).wait_recv()
    o_local.wait()


N_WIRES = 6 + 12 + 6 + 12 + 6 + 24 + 12 + 6


def attend_and_gather(mesh, layer, norm, n_heads, act, w_t, mods, kv, shards):
    n_tp, n_cfg = mesh.shape['tp'], mesh.shape['cfg']
    n_tok, dim = act.shape
    width = w_t.shape[1]
    head_dim = width // n_heads
    vmem = pl.BlockSpec(memory_space=pltpu.VMEM)
    hbm = pl.BlockSpec(memory_space=pl.ANY)
    sem = pltpu.SemaphoreType.DMA
    out_shape = [jax.ShapeDtypeStruct((n_tp, width, n_tok // n_tp), BF16)]
    out_shape += [jax.ShapeDtypeStruct((n_tp,) + shard.shape, BF16) for shard in (kv,) + shards]
    return pl.pallas_call(
        functools.partial(attn_kernel, n_tp, n_cfg, head_dim, head_dim ** -0.5, norm),
        out_shape=out_shape,
        in_specs=[hbm, vmem, vmem] + [hbm] * 6,
        out_specs=[hbm] * 7,
        scratch_shapes=[pltpu.VMEM((n_tp, width, n_tok // n_tp), BF16), pltpu.VMEM((n_tp, n_tok // n_tp, dim), BF16),
                        pltpu.VMEM((width, n_tok), BF16), pltpu.VMEM((n_tok, width), BF16), pltpu.VMEM((n_heads, head_dim + 8, n_tok), BF16),
                        sem((N_WIRES,)), sem((N_WIRES,)), sem((n_tp - 1,)), sem((n_tp - 1,)), sem, sem((n_tp,))],
        compiler_params=pltpu.CompilerParams(collective_id=layer, has_side_effects=True, vmem_limit_bytes=60 << 20),
        name=f'attend_gather_{layer}',
    )(act, w_t, mods, kv, *shards)


def mlp_kernel(res_ref, mod_ref, w1_ref, w2_ref, out_ref, next_ref, a_buf, total):
    at = pl.program_id(0)

    @pl.when(at == 0)
    def _():
        a_buf[...] = (layer_norm(res_ref[...]) * (1.0 + mod_ref[1:2]) + mod_ref[0:1]).astype(BF16)
        total[...] = jnp.zeros_like(total)
    hidden = lax.dot_general(a_buf[...], w1_ref[...], (((1,), (1,)), ((), ())), preferred_element_type=F32)
    hidden = jax.nn.gelu(hidden, approximate=True).astype(BF16)
    total[...] += jnp.dot(hidden, w2_ref[...], preferred_element_type=F32)

    @pl.when(at == pl.num_programs(0) - 1)
    def _():
        out = res_ref[...] + mod_ref[2:3] * total[...].astype(BF16).astype(F32)
        out_ref[...] = out
        next_ref[...] = (layer_norm(out) * (1.0 + mod_ref[4:5]) + mod_ref[3:4]).astype(BF16)


def mlp(residual, mods, w1, w2):
    n_own, dim = residual.shape
    whole = lambda shape: pl.BlockSpec(shape, lambda at: (0, 0))
    block = pl.BlockSpec((F_ROWS, dim), lambda at: (at, 0))
    return pl.pallas_call(
        mlp_kernel,
        grid=(w1.shape[0] // F_ROWS,),
        out_shape=[jax.ShapeDtypeStruct((n_own, dim), F32), jax.ShapeDtypeStruct((n_own, dim), BF16)],
        in_specs=[whole((n_own, dim)), whole(mods.shape), block, block],
        out_specs=[whole((n_own, dim)), whole((n_own, dim))],
        scratch_shapes=[pltpu.VMEM((n_own, dim), BF16), pltpu.VMEM((n_own, dim), F32)],
        compiler_params=pltpu.CompilerParams(vmem_limit_bytes=48 << 20),
        cost_estimate=pl.CostEstimate(flops=4 * n_own * dim * w1.shape[0], bytes_accessed=4 * dim * w1.shape[0], transcendentals=0),
        name='norm_mlp',
    )(residual, mods, w1, w2)


def final_kernel(n_tp, n_cfg, n_img, eps_ref, x_ref, co_ref, out_ref, pair_buf, send_buf, pair_send, pair_recv, send_sem, recv_sem):
    me = lax.axis_index('tp')
    row = lax.axis_index('cfg')
    pair, up, down = lax.rem(row + n_img, n_cfg), lax.rem(row + 1, n_cfg), lax.rem(row + n_cfg - 1, n_cfg)
    image = lax.rem(row, n_img)
    barrier = pltpu.get_barrier_semaphore()
    pl.semaphore_signal(barrier, inc=1, device_id={'cfg': pair}, device_id_type=MESH)
    for step in range(n_tp):
        tp = lax.rem(me + step, n_tp)
        if step:
            pl.semaphore_signal(barrier, inc=1, device_id={'tp': tp}, device_id_type=MESH)
        pl.semaphore_signal(barrier, inc=1, device_id={'cfg': down, 'tp': tp}, device_id_type=MESH)
    pl.semaphore_wait(barrier, 2 * n_tp)
    swap = pltpu.make_async_remote_copy(src_ref=eps_ref, dst_ref=pair_buf, send_sem=pair_send, recv_sem=pair_recv,
                                        device_id={'cfg': pair}, device_id_type=MESH)
    swap.start()
    swap.wait()
    is_cond = row < n_img
    mine, other = eps_ref[...], pair_buf[...]
    cond, uncond = jnp.where(is_cond, mine, other), jnp.where(is_cond, other, mine)
    guided = uncond + GUIDANCE * (cond - uncond)
    x_zero = (x_ref[...] - co_ref[0:1] * guided) / co_ref[1:2]
    result = co_ref[2:3] * x_zero + co_ref[3:4] * guided
    send_buf[...] = result
    out_ref[image, me] = result

    def chunk_copy(step, ring, origin, img, dev):
        k = step * 2 + ring
        return pltpu.make_async_remote_copy(src_ref=send_buf, dst_ref=out_ref.at[img, origin], send_sem=send_sem.at[k],
                                            recv_sem=recv_sem.at[k], device_id=dev, device_id_type=MESH)

    for ring in range(2):
        for step in range(1 - ring, n_tp):
            tp = lax.rem(me + step, n_tp)
            chunk_copy(step, ring, me, image, {'cfg': up, 'tp': tp} if ring else {'tp': tp}).start()
    for ring in range(2):
        for step in range(1 - ring, n_tp):
            origin = lax.rem(me + n_tp - step, n_tp)
            img = lax.rem(down, n_img) if ring else image
            dev = {'cfg': down, 'tp': origin} if ring else {'tp': origin}
            chunk_copy(step, ring, origin, img, dev).wait_recv()
            chunk_copy(step, ring, origin, img, dev).wait_send()


def final_step(mesh, eps, x_own, coef, n_img):
    n_tp, n_cfg = mesh.shape['tp'], mesh.shape['cfg']
    vmem = pl.BlockSpec(memory_space=pltpu.VMEM)
    sem = pltpu.SemaphoreType.DMA
    return pl.pallas_call(
        functools.partial(final_kernel, n_tp, n_cfg, n_img),
        out_shape=jax.ShapeDtypeStruct((n_img, n_tp) + eps.shape, F32),
        in_specs=[vmem] * 3,
        out_specs=vmem,
        scratch_shapes=[pltpu.VMEM(eps.shape, F32), pltpu.VMEM(eps.shape, F32), sem, sem, sem((2 * n_tp,)), sem((2 * n_tp,))],
        compiler_params=pltpu.CompilerParams(collective_id=16, has_side_effects=True),
        name='guide_and_share',
    )(eps, x_own, coef)


def gather_kernel(n_tp, x_ref, out_ref, send_sem, recv_sem, loc_sem):
    me = lax.axis_index('tp')
    east, west, opp = lax.rem(me + 2, n_tp), lax.rem(me + n_tp - 2, n_tp), lax.rem(me + 4, n_tp)
    flip = lambda idx: idx + 1 - 2 * lax.rem(idx, 2)
    mate = flip(me)
    to_east, to_west, to_mate = {'tp': east}, {'tp': west}, {'tp': mate}
    half = x_ref.shape[0] // 2
    barrier = pltpu.get_barrier_semaphore()
    for dev in (to_east, to_west, to_mate):
        pl.semaphore_signal(barrier, inc=1, device_id=dev, device_id_type=MESH)
    pl.semaphore_wait(barrier, 3)
    wires = Wires(send_sem, recv_sem)
    low, high = pl.ds(0, half), pl.ds(half, half)
    for tag, cut in (('l', low), ('h', high)):
        order = (('E', to_east), ('W', to_west)) if tag == 'l' else (('W', to_west), ('E', to_east))
        for side, dev in order:
            wires.start((side, tag), x_ref.at[cut], out_ref.at[me, cut], dev)
    wires.start(('own',), x_ref, out_ref.at[me], to_mate)
    local = pltpu.make_async_copy(x_ref, out_ref.at[me], loc_sem)
    local.start()
    wires.arrived(('E', 'l'), out_ref.at[west, low], to_west)
    part = out_ref.at[west, low]
    wires.start(('fE',), part, part, to_east)
    wires.start(('d', 'wl'), part, part, to_mate)
    wires.arrived(('W', 'h'), out_ref.at[east, high], to_east)
    part = out_ref.at[east, high]
    wires.start(('fW',), part, part, to_west)
    wires.start(('d', 'eh'), part, part, to_mate)
    for key, tag, part, dev in ((('E', 'h'), 'wh', out_ref.at[west, high], to_west), (('W', 'l'), 'el', out_ref.at[east, low], to_east),
                                (('fE',), 'ol', out_ref.at[opp, low], to_west), (('fW',), 'oh', out_ref.at[opp, high], to_east)):
        wires.arrived(key, part, dev)
        wires.start(('d', tag), part, part, to_mate)
    for shard, tag in ((west, 'w'), (east, 'e'), (opp, 'o')):
        wires.arrived(('d', tag + 'l'), out_ref.at[flip(shard), low], to_mate)
        wires.arrived(('d', tag + 'h'), out_ref.at[flip(shard), high], to_mate)
    wires.arrived(('own',), out_ref.at[mate], to_mate)
    wires.drain()
    local.wait()


def gather_tokens(mesh, layer, part):
    n_tp = mesh.shape['tp']
    sem = pltpu.SemaphoreType.DMA
    return pl.pallas_call(
        functools.partial(gather_kernel, n_tp),
        out_shape=jax.ShapeDtypeStruct((n_tp,) + part.shape, BF16),
        in_specs=[pl.BlockSpec(memory_space=pltpu.VMEM)],
        out_specs=pl.BlockSpec(memory_space=pl.ANY),
        scratch_shapes=[sem((13,)), sem((13,)), sem],
        compiler_params=pltpu.CompilerParams(collective_id=8 + layer, has_side_effects=True),
        name=f'gather_tokens_{layer}',
    )(part)


def solution(mesh):
    row_spec = P(('dp', 'cfg'))
    part_spec = P('dp')
    in_specs = (row_spec, row_spec, row_spec, part_spec, part_spec, part_spec, part_spec, P(),
                P(None, None, None, 'tp'), P(None, 'tp'), P(None, None, 'tp'), P(None, None, None, 'tp'),
                P(None, 'tp'), P(None, None, 'tp'), P(None, 'tp'), P(), P(), P())
    n_tp, n_cfg = mesh.shape['tp'], mesh.shape['cfg']

    def local_step(hidden, caption, cap_len, t_block, t_embed, x_t, alpha_bar, mod_table, w_qkv, w_proj, w_cq, w_ckv, w_cproj, w_fc1, w_fc2, final_table, w_out, b_out):
        _, n_tok, dim = hidden.shape
        n_layers, n_heads, head_dim = w_proj.shape[:3]
        width = n_heads * head_dim
        n_own = n_tok // n_tp
        n_text = caption.shape[1]
        n_img = t_block.shape[0]
        image = lax.axis_index('cfg') % n_img
        me = lax.axis_index('tp')
        t_rows = lax.dynamic_index_in_dim(t_block, image, keepdims=False).astype(F32).reshape(6, dim)
        emb_row = lax.dynamic_index_in_dim(t_embed, image, keepdims=False).astype(F32)
        key_mask = (jnp.arange(n_text) < cap_len[0])[None, None, :]
        residual = lax.dynamic_slice_in_dim(hidden[0], me * n_own, n_own).astype(F32)
        all_mods = mod_table.astype(F32) + t_rows[None]
        final_mods = final_table.astype(F32) + emb_row[None, :]
        attn_in = hidden[0]
        for layer in range(n_layers):
            mods = all_mods[layer]
            if layer:
                attn_in = gather_tokens(mesh, layer, next_in).reshape(n_tok, dim)
            w_t = w_qkv[layer].transpose(1, 2, 3, 0).reshape(3, width, dim)
            kv = dot32('td,dshe->shet', caption[0], w_ckv[layer]).astype(BF16).reshape(2 * n_heads, head_dim, n_text)
            f_rows = w_fc2.shape[1] // n_cfg
            shards = (w_proj[layer].reshape(width, dim), w_cq[layer].reshape(dim, width).T, w_cproj[layer].reshape(width, dim),
                      w_fc1[layer].T.reshape(n_cfg, f_rows, dim), w_fc2[layer].reshape(n_cfg, f_rows, dim))
            o_all, kv_all, g_proj, g_cq, g_cproj, g_fc1, g_fc2 = attend_and_gather(mesh, layer, layer == 0, n_heads, attn_in, w_t, mods, kv, shards)
            self_out = dot32('kn,kd->nd', o_all.reshape(n_tp * width, n_own), g_proj.reshape(n_tp * width, dim)).astype(BF16)
            residual = residual + mods[2] * self_out.astype(F32)
            cross_q = dot32('nd,hed->hne', residual.astype(BF16), g_cq.reshape(n_tp * n_heads, head_dim, dim)).astype(BF16)
            kv_all = kv_all.reshape(n_tp, 2, n_heads, head_dim, n_text)
            cross_k = kv_all[:, 0].reshape(n_tp * n_heads, head_dim, n_text)
            cross_v = kv_all[:, 1].reshape(n_tp * n_heads, head_dim, n_text)
            scores = dot32('hne,het->hnt', cross_q, cross_k) * head_dim ** -0.5
            scores = jnp.where(key_mask, scores, -1e30)
            probs = jax.nn.softmax(scores, axis=-1).astype(BF16)
            cross_o = dot32('hnt,het->nhe', probs, cross_v).astype(BF16)
            cross_out = dot32('nk,kd->nd', cross_o.reshape(n_own, n_tp * width), g_cproj.reshape(n_tp * width, dim)).astype(BF16)
            residual = residual + cross_out.astype(F32)
            after = all_mods[layer + 1, :2] if layer + 1 < n_layers else final_mods
            mlp_mods = jnp.concatenate([mods[3:6], after, jnp.zeros((3, dim), F32)], axis=0)
            n_ff = g_fc1.shape[0] * g_fc1.shape[1] * g_fc1.shape[2]
            residual, next_in = mlp(residual, mlp_mods, g_fc1.reshape(n_ff, dim), g_fc2.reshape(n_ff, dim))
        side = x_t.shape[1]
        grid = side // 2
        n_own_rows = n_own // grid
        out_tok = dot32('nd,dc->cn', next_in, w_out) + b_out.astype(F32)[:, None]
        eps = out_tok.reshape(2, 2, 8, n_own_rows, grid)[:, :, :4]
        place = (jnp.arange(side)[None, None, :] == 2 * jnp.arange(grid)[None, :, None] + jnp.arange(2)[:, None, None]).astype(F32)
        eps = jnp.einsum('pqcij,qjx->ipcx', eps, place, precision=lax.Precision.HIGHEST, preferred_element_type=F32)
        eps = eps.reshape(n_own_rows * 2 * 4, side)
        x_rows = x_t.transpose(0, 1, 3, 2).reshape(n_img, n_tp, n_own_rows * 2 * 4, side)
        x_own = lax.dynamic_slice(x_rows, (image, me, 0, 0), (1, 1) + x_rows.shape[2:])[0, 0]
        abar = lax.dynamic_index_in_dim(alpha_bar, image, keepdims=False)
        coef = jnp.stack([jnp.sqrt(1.0 - abar[0]), jnp.sqrt(abar[0]), jnp.sqrt(abar[1]), jnp.sqrt(1.0 - abar[1])])
        coef = jnp.broadcast_to(jnp.concatenate([coef, coef])[:, None], (8, side))
        x_prev = final_step(mesh, eps, x_own, coef, n_img)
        return x_prev.reshape(n_img, side, 4, side).transpose(0, 1, 3, 2)

    return jax.shard_map(local_step, mesh=mesh, in_specs=in_specs, out_specs=part_spec, check_vma=False)
```
